32 devices in a mesh: dp: 8 (over z, x), tensor: 4 (over y, core).
Axes of the slice: x: 2, y: 2, z: 4, core: 2. Of those that a mesh axis runs over, the one named last changes fastest.
Arguments:
- out_first: bfloat16 [8, 197, 1024], P('dp', None, 'tensor'), may hold values from -6 to 6
- out_second: bfloat16 [8, 197, 1024], P('dp', None, 'tensor'), may hold values from -6 to 6
- grad_first: bfloat16 [8, 197, 1024], P('dp', None, 'tensor'), may hold values from -6 to 6
- grad_second: bfloat16 [8, 197, 1024], P('dp', None, 'tensor'), may hold values from -6 to 6
- gain_attn: float32 [1024], replicated, may hold values from 0.25 to 1.75
- gain_mlp: float32 [1024], replicated, may hold values from 0.25 to 1.75
- qkv_weight: bfloat16 [1024, 3, 1024], P(None, None, 'tensor'), may hold values from -1 to 1
- proj_weight: bfloat16 [1024, 1024], P(None, 'tensor'), may hold values from -0.1875 to 0.1875
- inner_weight: bfloat16 [1024, 4096], P(None, 'tensor'), may hold values from -0.1875 to 0.1875
- inner_bias: float32 [4096], P('tensor'), may hold values from -3 to 3
- outer_weight: bfloat16 [1024, 4096], P(None, 'tensor'), may hold values from -0.09375 to 0.09375
Outputs:
- input_first: bfloat16 [8, 197, 1024], P('dp', None, 'tensor')
- input_second: bfloat16 [8, 197, 1024], P('dp', None, 'tensor')
- back_first: bfloat16 [8, 197, 1024], P('dp', None, 'tensor')
- back_second: bfloat16 [8, 197, 1024], P('dp', None, 'tensor')
- grad_qkv: float32 [1024, 3, 1024], P('dp', None, 'tensor')
- grad_proj: float32 [1024, 1024], P('dp', 'tensor')
- grad_inner: float32 [1024, 4096], P('dp', 'tensor')
- grad_bias: float32 [4096], P('tensor')
- grad_outer: float32 [1024, 4096], P('dp', 'tensor')
- grad_gain_attn: float32 [1024], P('tensor')
- grad_gain_mlp: float32 [1024], P('tensor')
The draws below stay inside these ranges and needn't reach their ends.
All inputs are finite; a program needn't handle non-finite values.
Results may differ from the reference program's by a relative error of at most 0.016.
Values may be sent and summed in bfloat16 or wider, within the bound.
A program may use at most 64 MiB of HBM per device.

```python
import jax
import jax.numpy as jnp
from jax import lax

D = 1024
HEADS = 16
FF = 4096
SEQ = 197
IMAGES = 8


def draw_qkv_weight(key, part):
    base_key = jax.random.fold_in(key, 0)
    base_draw = jax.random.truncated_normal(base_key, -6.0, 6.0, (D, 3, D), jnp.float32) / D ** 0.5
    return jnp.clip(base_draw, -1.0, 1.0).astype(jnp.bfloat16)


def strengthened(array, own_key, source, target, blocks, factor):
    def block_of(axis_at):
        return (jnp.arange(array.shape[axis_at]) // (array.shape[axis_at] // blocks)).reshape((-1,) + (1,) * (array.ndim - 1 - axis_at))

    first = jax.random.permutation(own_key, blocks)[block_of(target)]
    other_side = (block_of(target) + blocks // 2) % blocks
    return jnp.where((block_of(source) == first) | (block_of(source) == other_side), factor * array, array)


def steps_of(key, shape, cuts, least, high):
    level = 1.0
    for axis_at, shards_of in cuts:
        heights = jax.random.uniform(jax.random.fold_in(jax.random.fold_in(key, 6), axis_at), (shards_of,), jnp.float32, least / len(cuts), high / len(cuts))
        level = level * jnp.repeat(jnp.exp(heights), shape[axis_at] // shards_of).reshape((-1,) + (1,) * (len(shape) - 1 - axis_at))
    return level


def noise(rng, shape, deviation, limit, cuts=(), dtype=jnp.bfloat16):
    values = jax.random.normal(rng, shape, jnp.float32) * deviation
    if len(cuts) > 0:
        values = steps_of(rng, shape, cuts, -0.22, 0.18) * values
    return jnp.clip(values, min=-limit, max=limit).astype(dtype)


def heavy_noise(own_key, shape, deviation, limit, pieces, heavy, kind=jnp.bfloat16):
    array = deviation * jax.random.normal(own_key, shape, jnp.float32)
    if pieces:
        array = array * steps_of(own_key, shape, pieces, -0.22, 0.18)
    return jnp.clip(strengthened(array, jax.random.fold_in(own_key, 3), *heavy), -limit, limit).astype(kind)


def setup_inputs(seed: int = 0) -> dict:
    keys = jax.random.split(jax.random.key(seed), 12)
    out_first = noise(keys[0], (IMAGES, SEQ, D), 1.0, 6.0, ((0, 8), (2, 4)))
    out_second = noise(keys[1], (IMAGES, SEQ, D), 1.0, 6.0, ((0, 8), (2, 4)))
    grad_first = noise(keys[2], (IMAGES, SEQ, D), 1.0, 6.0, ((0, 8), (2, 4)))
    grad_second = heavy_noise(keys[3], (IMAGES, SEQ, D), 1.0, 6.0, ((0, 8), (2, 4)), (0, 2, 8, 2.0))
    gain_attn = jnp.clip(1.0 + 0.15 * jax.random.normal(keys[4], (D,), jnp.float32), 0.25, 1.75)
    gain_mlp = jnp.clip(1.0 + 0.15 * jax.random.normal(keys[5], (D,), jnp.float32), 0.25, 1.75)
    qkv_weight = draw_qkv_weight(jax.random.fold_in(keys[11], 71), 0)
    proj_weight = noise(keys[7], (D, D), D ** -0.5, 0.1875, ((1, 4),))
    inner_weight = noise(keys[8], (D, FF), D ** -0.5, 0.1875, ((1, 4),))
    inner_bias = noise(keys[9], (FF,), 0.5, 3.0, ((0, 4),), jnp.float32)
    outer_weight = noise(keys[10], (D, FF), FF ** -0.5, 0.09375, ((1, 4),))
    return {"out_first": out_first, "out_second": out_second, "grad_first": grad_first, "grad_second": grad_second, "gain_attn": gain_attn, "gain_mlp": gain_mlp, "qkv_weight": qkv_weight, "proj_weight": proj_weight, "inner_weight": inner_weight, "inner_bias": inner_bias, "outer_weight": outer_weight}


epsilon = 1e-06

def normalize(values):
    centre = values - lax.optimization_barrier(jnp.mean(values, -1, keepdims=True))
    spread = lax.rsqrt(lax.optimization_barrier(jnp.mean(centre * centre, -1, keepdims=True)) + epsilon)
    return (centre * spread, spread)

def norm_back(grad_in, normed, spread, gain):
    scaled = grad_in * gain
    first_mean = lax.optimization_barrier(jnp.mean(scaled, -1, keepdims=True))
    second_mean = lax.optimization_barrier(jnp.mean(scaled * normed, -1, keepdims=True))
    return spread * (scaled - first_mean - normed * second_mean)

def image_attention(members):
    queries = members[0].astype(jnp.float32)
    key_rows = members[1].astype(jnp.float32)
    value_rows = members[2].astype(jnp.float32)
    grad_heads = members[3].astype(jnp.float32)
    factor = (D // HEADS) ** (-0.5)
    scores = jnp.einsum('qhe,khe->hqk', queries, key_rows) * factor
    attn_probs = jax.nn.softmax(scores, -1)
    probs_low = attn_probs.astype(jnp.bfloat16)
    probs_wide = probs_low.astype(jnp.float32)
    heads_out = jnp.einsum('hqk,khe->qhe', probs_wide, value_rows).astype(jnp.bfloat16)
    grad_probs = jnp.einsum('qhe,khe->hqk', grad_heads, value_rows)
    grad_value = jnp.einsum('hqk,qhe->khe', probs_wide, grad_heads).astype(jnp.bfloat16)
    row_dot = lax.optimization_barrier(jnp.sum(grad_probs * attn_probs, -1, keepdims=True))
    grad_scores = (attn_probs * (grad_probs - row_dot)).astype(jnp.bfloat16).astype(jnp.float32)
    grad_query = (jnp.einsum('hqk,khe->qhe', grad_scores, key_rows) * factor).astype(jnp.bfloat16)
    grad_key = (jnp.einsum('hqk,qhe->khe', grad_scores, queries) * factor).astype(jnp.bfloat16)
    return (heads_out, grad_query, grad_key, grad_value)

def reference(out_first, out_second, grad_first, grad_second, gain_attn, gain_mlp, qkv_weight, proj_weight, inner_weight, inner_bias, outer_weight):
    rows_all = IMAGES * SEQ
    head_dim = D // HEADS
    first_rows = out_first.reshape(rows_all, D).astype(jnp.float32)
    second_rows = out_second.reshape(rows_all, D).astype(jnp.float32)
    upper_grad = grad_first.reshape(rows_all, D).astype(jnp.float32)
    lower_grad = grad_second.reshape(rows_all, D)
    normed_mlp, spread_mlp = normalize(first_rows)
    input_mlp = (normed_mlp * gain_mlp).astype(jnp.bfloat16)
    hidden = jnp.dot(input_mlp, inner_weight, preferred_element_type=jnp.float32) + inner_bias
    active = jax.nn.gelu(hidden).astype(jnp.bfloat16)
    mlp_out = jnp.dot(active, outer_weight.T, preferred_element_type=jnp.float32)
    input_second = (second_rows - mlp_out).astype(jnp.bfloat16)
    grad_active = jnp.dot(lower_grad, outer_weight, preferred_element_type=jnp.float32)
    grad_hidden = jax.vjp(jax.nn.gelu, hidden)[1](grad_active)[0].astype(jnp.bfloat16)
    grad_outer = jnp.dot(lower_grad.T, active, preferred_element_type=jnp.float32)
    grad_inner = jnp.dot(input_mlp.T, grad_hidden, preferred_element_type=jnp.float32)
    grad_bias = lax.optimization_barrier(jnp.sum(grad_hidden.astype(jnp.float32), 0))
    grad_norm_mlp = jnp.dot(grad_hidden, inner_weight.T, preferred_element_type=jnp.float32)
    grad_gain_mlp = lax.optimization_barrier(jnp.sum(grad_norm_mlp * normed_mlp, 0))
    back_first = (upper_grad + norm_back(grad_norm_mlp, normed_mlp, spread_mlp, gain_mlp)).astype(jnp.bfloat16)
    normed_attn, spread_attn = normalize(input_second.astype(jnp.float32))
    input_attn = (normed_attn * gain_attn).astype(jnp.bfloat16)
    qkv_rows = jnp.einsum('td,dcj->tcj', input_attn.astype(jnp.float32), qkv_weight.astype(jnp.float32)).astype(jnp.bfloat16)
    grad_heads = jnp.dot(back_first, proj_weight, preferred_element_type=jnp.float32).astype(jnp.bfloat16)
    shaped = qkv_rows.reshape(IMAGES, SEQ, 3, HEADS, head_dim)
    heads_out, grad_query, grad_key, grad_value = lax.map(image_attention, (shaped[:, :, 0], shaped[:, :, 1], shaped[:, :, 2], grad_heads.reshape(IMAGES, SEQ, HEADS, head_dim)))
    attn_rows = heads_out.reshape(rows_all, D)
    grad_rows = jnp.stack([grad_query, grad_key, grad_value], 2).reshape(rows_all, 3, D)
    attn_out = jnp.dot(attn_rows, proj_weight.T, preferred_element_type=jnp.float32)
    input_first = (first_rows - attn_out).astype(jnp.bfloat16)
    grad_proj = jnp.dot(back_first.T, attn_rows, preferred_element_type=jnp.float32)
    grad_qkv = jnp.einsum('td,tcj->dcj', input_attn.astype(jnp.float32), grad_rows.astype(jnp.float32))
    grad_norm_attn = jnp.einsum('tcj,dcj->td', grad_rows.astype(jnp.float32), qkv_weight.astype(jnp.float32))
    grad_gain_attn = lax.optimization_barrier(jnp.sum(grad_norm_attn * normed_attn, 0))
    back_second = (lower_grad.astype(jnp.float32) + norm_back(grad_norm_attn, normed_attn, spread_attn, gain_attn)).astype(jnp.bfloat16)
    shape_out = (IMAGES, SEQ, D)
    return (input_first.reshape(shape_out), input_second.reshape(shape_out), back_first.reshape(shape_out), back_second.reshape(shape_out), grad_qkv, grad_proj, grad_inner, grad_bias, grad_outer, grad_gain_attn, grad_gain_mlp)
```

```python
import functools

import jax
import jax.numpy as jnp
from jax import lax
from jax.experimental import pallas as pl
from jax.experimental.pallas import tpu as pltpu
from jax.sharding import PartitionSpec as P

epsilon = 1e-06
HEAD = 64
BF = jnp.bfloat16
F32 = jnp.float32
MESH = pl.DeviceIdType.MESH


def dot(a, b, dims=((1,), (0,))):
    return lax.dot_general(a, b, (dims, ((), ())), preferred_element_type=F32)


NT = ((1,), (1,))
TN = ((0,), (0,))


def kernel(
    sizes,
    of_ref, os_ref, gf_ref, gs_ref, gain_attn, gain_mlp, bias,
    qkv_hbm, proj_hbm, inner_hbm, outer_hbm,
    o_if, o_is, o_bf, o_bs, o_qkv, o_proj, o_inner, o_small, o_outer,
    w_qkv, w_proj, w_inner, w_outer,
    g_of, g_low, g_gf, g_is, g_gn, g_gna,
    a_mlp, a_attn, a_back, n_mlp, n_attn, sp_attn,
    dgelu, qkv, gheads,
    at, lr,
    r_act, r_gh, r_attn, r_rows,
    rs_s1, rs_r1, rs_k, rs_s2, rs_r2,
    sm_s, sm_r,
    *rest,
):
    groups, length, width, full, hid, tile, rows = sizes
    bits = groups.bit_length() - 1
    shard = full // groups
    pieces = rest[:-3]
    ssem, rsem, wsem = rest[-3:]
    d = lax.axis_index("dp")
    me = lax.axis_index("tensor")
    core, yy = me % 2, me // 2
    tc = yy * 2 + 1 - core
    ty = (1 - yy) * 2 + core
    td = (1 - yy) * 2 + 1 - core
    bit = [(d // 2**k) % 2 for k in range(bits)]
    partner = [d + (1 - 2 * bit[k]) * 2**k for k in range(bits)]
    counter = [0]
    pending = []

    def send(src, dst, dp_id, t_id):
        k = counter[0]
        counter[0] += 1
        c = pltpu.make_async_remote_copy(
            src_ref=src, dst_ref=dst, send_sem=ssem.at[k], recv_sem=rsem.at[k],
            device_id=(dp_id, t_id), device_id_type=MESH,
        )
        c.start()
        pending.append(c)
        return c

    def cols(i):
        return pl.ds(pl.multiple_of(i * width, width), width)

    weights = []
    for i, (src, dst) in enumerate(
        [(inner_hbm, w_inner), (outer_hbm, w_outer), (qkv_hbm, w_qkv), (proj_hbm, w_proj)]
    ):
        c = pltpu.make_async_copy(src, dst, wsem.at[i])
        c.start()
        weights.append(c)

    barrier = pltpu.get_barrier_semaphore()
    peers = [(d, tc), (d, ty)] + [(p, me) for p in partner]
    for peer in peers:
        pl.semaphore_signal(barrier, inc=1, device_id=peer, device_id_type=MESH)

    def stage(g, src):
        g[:, cols(me)] = jnp.zeros((rows, width), BF)
        g[0:length, cols(me)] = src[0]

    stage(g_of, of_ref)
    stage(g_low, gs_ref)
    stage(g_gf, gf_ref)
    pl.semaphore_wait(barrier, len(peers))

    def ag_start(g):
        own = g.at[:, cols(me)]
        c2 = send(own, own, d, ty)
        c1 = send(own, own, d, tc)
        return [c1, c2]

    def ag_mid(g, cs):
        cs[1].wait_recv()
        far = g.at[:, cols(ty)]
        cs.append(send(far, far, d, tc))

    def ag_end(cs):
        cs[0].wait_recv()
        cs[2].wait_recv()

    def rs_start(i, part):
        rs_s1[i, 0] = part(tc).astype(BF)
        c0 = send(rs_s1.at[i, 0], rs_r1.at[i, 0], d, tc)
        rs_s1[i, 1] = part(td).astype(BF)
        c1 = send(rs_s1.at[i, 1], rs_r1.at[i, 1], d, tc)
        rs_k[i, 1] = part(ty)
        rs_k[i, 0] = part(me)
        return [c0, c1]

    def rs_mid(i, cs):
        cs[1].wait_recv()
        rs_s2[i] = (rs_k[i, 1] + rs_r1[i, 1].astype(F32)).astype(BF)
        cs.append(send(rs_s2.at[i], rs_r2.at[i], d, ty))

    def rs_end(i, cs):
        cs[0].wait_recv()
        cs[2].wait_recv()
        return rs_k[i, 0] + rs_r1[i, 0].astype(F32) + rs_r2[i].astype(F32)

    def normalize(values):
        centre = values - jnp.mean(values, -1, keepdims=True)
        spread = lax.rsqrt(jnp.mean(centre * centre, -1, keepdims=True) + epsilon)
        return centre * spread, spread

    def left(i, a):
        t = a[...].T
        at[i] = t.reshape(groups // 2, 2, shard, rows)
        return send(at.at[i, :, 1 - bit[0]], lr.at[i], partner[0], me)

    def right(r):
        return send(r.at[0], r.at[1], partner[0], me)

    def piece(p, i, r, cl, cr):
        cl.wait_recv()
        cr.wait_recv()
        bufs = pieces[p]
        n = r.shape[2]
        m = groups // 2
        mine = at[i, :, bit[0]].reshape(m * shard, rows)
        theirs = lr[i].reshape(m * shard, rows)
        for j in range(n // width):
            c = slice(j * width, (j + 1) * width)
            acc = dot(mine, r[0, :, c]) + dot(theirs, r[1, :, c])
            bufs[0][:, :, :, c] = acc.reshape(m // 2, 2, shard, width)
        return halve(p, 1)

    def halve(p, k):
        keep, s, r = pieces[p][3 * (k - 1) : 3 * k]
        s[...] = keep[:, 1 - bit[k]].astype(BF)
        return send(s, r, partner[k], me)

    def merge(p, k, c, out=None):
        c.wait_recv()
        keep, s, r = pieces[p][3 * (k - 1) : 3 * k]
        total = keep[:, bit[k]] + r[...].astype(F32)
        if k == bits - 1:
            out[...] = total[0]
            return None
        nxt = pieces[p][3 * k]
        nxt[...] = total.reshape(nxt.shape)
        return halve(p, k + 1)

    c_of = ag_start(g_of)
    c_low = ag_start(g_low)
    ag_mid(g_of, c_of)
    ag_end(c_of)
    normed, sp_mlp = normalize(g_of[...].astype(F32))
    n_mlp[...] = normed
    a_mlp[...] = (normed * gain_mlp[...]).astype(BF)
    ag_mid(g_low, c_low)
    c_gf = ag_start(g_gf)

    weights[0].wait()
    for j in range(hid // tile):
        c = slice(j * tile, (j + 1) * tile)
        h = dot(a_mlp[...], w_inner[:, c]) + bias[:, c]
        k0, k1 = 0.7978845608028654, 0.044715
        sq = h * h
        t = jnp.tanh(k0 * h * (1.0 + k1 * sq))
        r_act[0, :, c] = (0.5 * h * (1.0 + t)).astype(BF)
        dgelu[:, c] = 0.5 * (1.0 + t) + 0.5 * h * (1.0 - t * t) * (k0 * (1.0 + 3.0 * k1 * sq))
    ag_end(c_low)
    x_low = left(0, g_low)
    x_act = right(r_act)
    weights[1].wait()
    c_mlp = rs_start(0, lambda i: dot(r_act[0], w_outer[cols(i), :], NT))
    ag_mid(g_gf, c_gf)
    for j in range(hid // tile):
        c = slice(j * tile, (j + 1) * tile)
        gh = dot(g_low[...], w_outer[:, c]) * dgelu[:, c]
        gl = gh.astype(BF)
        r_gh[0, :, c] = gl
        sm_s[0, :, 2 * width + j * tile : 2 * width + (j + 1) * tile] = jnp.sum(
            gl.astype(F32), 0, keepdims=True
        )
    x_mlp = left(1, a_mlp)
    x_gh = right(r_gh)
    rs_mid(0, c_mlp)
    c_gn = rs_start(1, lambda i: dot(r_gh[0], w_inner[cols(i), :], NT))
    total = rs_end(0, c_mlp)
    second = (os_ref[0].astype(F32) - total[0:length]).astype(BF)
    o_is[0] = second
    g_is[:, cols(me)] = jnp.zeros((rows, width), BF)
    g_is[0:length, cols(me)] = second
    c_is = ag_start(g_is)
    rs_mid(1, c_gn)
    ag_mid(g_is, c_is)
    total = rs_end(1, c_gn)
    g_gn[:, cols(me)] = total.astype(BF)
    c_ggn = ag_start(g_gn)
    sm_s[0, :, width : 2 * width] = jnp.sum(total * n_mlp[:, cols(me)], 0, keepdims=True)
    ag_end(c_is)
    normed, spread = normalize(g_is[...].astype(F32))
    n_attn[...] = normed
    sp_attn[...] = jnp.broadcast_to(spread, sp_attn.shape)
    a_attn[...] = (normed * gain_attn[...]).astype(BF)
    ag_mid(g_gn, c_ggn)
    weights[2].wait()
    for j in range(3):
        c = slice(j * width, (j + 1) * width)
        qkv[:, c] = dot(a_attn[...], w_qkv[:, c]).astype(BF)
    ag_end(c_gf)
    ag_end(c_ggn)

    def means(g, n, gain):
        scaled = g * gain
        return (
            jnp.mean(scaled, -1, keepdims=True),
            jnp.mean(scaled * n, -1, keepdims=True),
        )

    g = g_gn[...].astype(F32)
    first, other = means(g, n_mlp[...], gain_mlp[...])
    back = sp_mlp * (g * gain_mlp[...] - first - n_mlp[...] * other)
    a_back[...] = (g_gf[...].astype(F32) + back).astype(BF)
    o_bf[0] = a_back[0:length, cols(me)]
    weights[3].wait()
    gheads[...] = dot(a_back[...], w_proj[...]).astype(BF)
    z_outer = piece(0, 0, r_act, x_low, x_act)

    factor = HEAD**-0.5
    valid = lax.broadcasted_iota(jnp.int32, (rows, rows), 1) < length
    for h in range(width // HEAD):
        c = slice(h * HEAD, (h + 1) * HEAD)
        q = qkv[:, c]
        k = qkv[:, width + h * HEAD : width + (h + 1) * HEAD]
        v = qkv[:, 2 * width + h * HEAD : 2 * width + (h + 1) * HEAD]
        gh = gheads[:, c]
        s = jnp.where(valid, dot(q, k, NT) * factor, -1e30)
        e = jnp.exp(s - jnp.max(s, -1, keepdims=True))
        p = e / jnp.sum(e, -1, keepdims=True)
        low = p.astype(BF)
        r_attn[0, :, c] = dot(low, v).astype(BF)
        gp = dot(gh, v, NT)
        gs = (p * (gp - jnp.sum(gp * p, -1, keepdims=True))).astype(BF)
        r_rows[0, :, c] = (dot(gs, k) * factor).astype(BF)
        r_rows[0, :, width + h * HEAD : width + (h + 1) * HEAD] = (
            dot(gs, q, TN) * factor
        ).astype(BF)
        r_rows[0, :, 2 * width + h * HEAD : 2 * width + (h + 1) * HEAD] = dot(low, gh, TN).astype(BF)
    x_rows = right(r_rows)
    x_attn = left(2, a_attn)
    x_attn_rows = right(r_attn)
    x_back = left(3, a_back)
    c_gna = rs_start(3, lambda i: dot(r_rows[0], w_qkv[cols(i), :], NT))
    c_out = rs_start(2, lambda i: dot(r_attn[0], w_proj[cols(i), :], NT))
    z_inner = piece(1, 1, r_gh, x_mlp, x_gh)
    rs_mid(3, c_gna)
    rs_mid(2, c_out)
    zs = [z_outer, z_inner]
    outs = [o_outer, o_inner, o_qkv, o_proj]
    zs[0] = merge(0, 1, zs[0], o_outer)
    total = rs_end(3, c_gna)
    g_gna[:, cols(me)] = total.astype(BF)
    c_ggna = ag_start(g_gna)
    sm_s[0, :, 0:width] = jnp.sum(total * n_attn[:, cols(me)], 0, keepdims=True)
    c_sm = send(sm_s.at[0], sm_r.at[0], partner[0], me)
    total = rs_end(2, c_out)
    o_if[0] = (of_ref[0].astype(F32) - total[0:length]).astype(BF)
    ag_mid(g_gna, c_ggna)
    zs.append(piece(2, 2, r_rows, x_attn, x_rows))
    zs.append(piece(3, 3, r_attn, x_back, x_attn_rows))
    ag_end(c_ggna)
    first, other = means(g_gna[...].astype(F32), n_attn[...], gain_attn[...])
    back = sp_attn[:, 0:1] * (
        g_gna[:, cols(me)].astype(F32) * gain_attn[:, cols(me)]
        - first
        - n_attn[:, cols(me)] * other
    )
    o_bs[0] = (gs_ref[0].astype(F32) + back[0:length]).astype(BF)
    done = [1, 0, 0, 0]
    for k in range(1, bits):
        c_sm.wait_recv()
        sm_s[k] = sm_s[k - 1] + sm_r[k - 1]
        c_sm = send(sm_s.at[k], sm_r.at[k], partner[k], me)
        for p in range(4):
            if done[p] < k:
                zs[p] = merge(p, k, zs[p], outs[p])
    if bits > 1:
        pass
    zs[0] = zs[0]
    c_sm.wait_recv()
    o_small[...] = sm_s[bits - 1] + sm_r[bits - 1]
    for c in pending:
        c.wait_send()


def on_device(
    out_first, out_second, grad_first, grad_second, gain_attn, gain_mlp,
    qkv_weight, proj_weight, inner_weight, inner_bias, outer_weight,
):
    images, length, width = out_first.shape
    parts = lax.axis_size("tensor")
    groups = lax.axis_size("dp")
    full = width * parts
    hid = inner_weight.shape[1]
    rows = (length + 15) // 16 * 16
    shard = full // groups
    bits = groups.bit_length() - 1
    sizes = (groups, length, width, full, hid, 256, rows)
    vm = pltpu.VMEM
    half = groups // 2
    scratch = [
        vm((full, 3 * width), BF), vm((full, width), BF), vm((full, hid), BF), vm((full, hid), BF),
    ]
    scratch += [vm((rows, full), BF)] * 6
    scratch += [vm((rows, full), BF)] * 3
    scratch += [vm((rows, full), F32)] * 2 + [vm((rows, 128), F32)]
    scratch += [vm((rows, hid), F32), vm((rows, 3 * width), BF), vm((rows, width), BF)]
    scratch += [vm((4, half, 2, shard, rows), BF), vm((4, half, shard, rows), BF)]
    scratch += [vm((2, rows, hid), BF), vm((2, rows, hid), BF), vm((2, rows, width), BF), vm((2, rows, 3 * width), BF)]
    scratch += [
        vm((4, 2, rows, width), BF), vm((4, 2, rows, width), BF), vm((4, 2, rows, width), F32),
        vm((4, rows, width), BF), vm((4, rows, width), BF),
    ]
    small = 2 * width + hid
    scratch += [vm((bits, 1, small), F32), vm((bits, 1, small), F32)]
    for n in (hid, hid, 3 * width, width):
        m = half
        bufs = []
        for k in range(1, bits):
            bufs += [vm((m // 2, 2, shard, n), F32), vm((m // 2, shard, n), BF), vm((m // 2, shard, n), BF)]
            m //= 2
        scratch.append(bufs)
    scratch += [pltpu.SemaphoreType.DMA((80,)), pltpu.SemaphoreType.DMA((80,)), pltpu.SemaphoreType.DMA((4,))]
    local = jax.ShapeDtypeStruct((images, length, width), BF)
    out_shape = [
        local, local, local, local,
        jax.ShapeDtypeStruct((shard, 3 * width), F32),
        jax.ShapeDtypeStruct((shard, width), F32),
        jax.ShapeDtypeStruct((shard, hid), F32),
        jax.ShapeDtypeStruct((1, small), F32),
        jax.ShapeDtypeStruct((shard, hid), F32),
    ]
    v = pl.BlockSpec(memory_space=pltpu.VMEM)
    a = pl.BlockSpec(memory_space=pl.ANY)
    o = pl.pallas_call(
        functools.partial(kernel, sizes),
        out_shape=out_shape,
        in_specs=[v] * 7 + [a] * 4,
        out_specs=[v] * 9,
        scratch_shapes=scratch,
        compiler_params=pltpu.CompilerParams(
            collective_id=0, has_side_effects=True, vmem_limit_bytes=60 * 2**20
        ),
    )(
        out_first, out_second, grad_first, grad_second,
        gain_attn.reshape(1, full), gain_mlp.reshape(1, full), inner_bias.reshape(1, hid),
        qkv_weight.reshape(full, 3 * width), proj_weight, inner_weight, outer_weight,
    )
    sums = o[7][0]
    return (
        o[0], o[1], o[2], o[3], o[4].reshape(shard, 3, width), o[5], o[6],
        sums[2 * width :], o[8], sums[:width], sums[width : 2 * width],
    )


def solution(mesh):
    act = P("dp", None, "tensor")
    in_specs = (
        act, act, act, act, P(), P(), P(None, None, "tensor"), P(None, "tensor"),
        P(None, "tensor"), P("tensor"), P(None, "tensor"),
    )
    out_specs = (
        act, act, act, act, P("dp", None, "tensor"), P("dp", "tensor"), P("dp", "tensor"),
        P("tensor"), P("dp", "tensor"), P("tensor"), P("tensor"),
    )
    return jax.shard_map(
        on_device, mesh=mesh, in_specs=in_specs, out_specs=out_specs, check_vma=False
    )
```

```python
import functools

import jax
import jax.numpy as jnp
from jax import lax
from jax.experimental import pallas as pl
from jax.experimental.pallas import tpu as pltpu
from jax.sharding import PartitionSpec as P

epsilon = 1e-06
HEAD = 64
BF = jnp.bfloat16
F32 = jnp.float32
MESH = pl.DeviceIdType.MESH


def dot(a, b, dims=((1,), (0,))):
    return lax.dot_general(a, b, (dims, ((), ())), preferred_element_type=F32)


NT = ((1,), (1,))
TN = ((0,), (0,))


def kernel(
    sizes,
    of_ref, os_ref, gf_ref, gs_ref, gain_attn, gain_mlp, bias,
    qkv_hbm, proj_hbm, inner_hbm, outer_hbm,
    o_if, o_is, o_bf, o_bs, o_qkv, o_proj, o_inner, o_ga, o_gm, o_bias, o_outer,
    w_qkv, w_proj, w_inner, w_outer,
    g_in, g_gf, g_is, g_gn, g_gna,
    a_mlp, a_more, a_attn, a_back, n_mlp, n_attn, sp_attn,
    dgelu, qkv, gheads,
    at, lr, atm, at_tmp,
    r_act, r_gh, r_attn, r_rows,
    rs_s1, rs_r1, rs_k, rs_s2, rs_r2,
    sm_s, sm_r,
    *rest,
):
    groups, length, width, full, hid, tile, rows = sizes
    bits = groups.bit_length() - 1
    shard = full // groups
    pieces = rest[:-3]
    ssem, rsem, wsem = rest[-3:]
    d = lax.axis_index("dp")
    me = lax.axis_index("tensor")
    core, yy = me % 2, me // 2
    tc = yy * 2 + 1 - core
    ty = (1 - yy) * 2 + core
    td = (1 - yy) * 2 + 1 - core
    bit = [(d // 2**k) % 2 for k in range(bits)]
    partner = [d + (1 - 2 * bit[k]) * 2**k for k in range(bits)]
    counter = [0]
    pending = []

    def send(src, dst, dp_id, t_id):
        k = counter[0]
        counter[0] += 1
        c = pltpu.make_async_remote_copy(
            src_ref=src, dst_ref=dst, send_sem=ssem.at[k], recv_sem=rsem.at[k],
            device_id=(dp_id, t_id), device_id_type=MESH,
        )
        c.start()
        pending.append(c)
        return c

    def cols(i):
        return pl.ds(pl.multiple_of(i * width, width), width)

    weights = []
    for i, (src, dst) in enumerate(
        [(inner_hbm, w_inner), (outer_hbm, w_outer), (qkv_hbm, w_qkv), (proj_hbm, w_proj)]
    ):
        c = pltpu.make_async_copy(src, dst, wsem.at[i])
        c.start()
        weights.append(c)

    barrier = pltpu.get_barrier_semaphore()
    both = partner[0] + (1 - 2 * bit[1]) * 2
    peers = [(d, tc), (d, ty), (both, me)] + [(p, me) for p in partner]
    for peer in peers:
        pl.semaphore_signal(barrier, inc=1, device_id=peer, device_id_type=MESH)

    def stage(g, src):
        g[:, cols(me)] = jnp.zeros((rows, width), BF)
        g[0:length, cols(me)] = src[0]

    g_of, g_low = g_in.at[0, 0], g_in.at[0, 1]
    stage(g_of, of_ref)
    stage(g_low, gs_ref)
    stage(g_gf, gf_ref)
    pl.semaphore_wait(barrier, len(peers))

    def part_of(g, i):
        return g.at[:, cols(i)] if len(g.shape) == 2 else g.at[:, :, cols(i)]

    def ag_start(g):
        own = part_of(g, me)
        c2 = send(own, own, d, ty)
        c1 = send(own, own, d, tc)
        return [c1, c2]

    def ag_mid(g, cs):
        cs[1].wait_recv()
        far = part_of(g, ty)
        cs.append(send(far, far, d, tc))

    def ag_end(cs):
        cs[0].wait_recv()
        cs[2].wait_recv()

    def rs_start(i, part):
        rs_s1[i, 0] = part(tc).astype(BF)
        c0 = send(rs_s1.at[i, 0], rs_r1.at[i, 0], d, tc)
        rs_s1[i, 1] = part(td).astype(BF)
        c1 = send(rs_s1.at[i, 1], rs_r1.at[i, 1], d, tc)
        rs_k[i, 1] = part(ty)
        rs_k[i, 0] = part(me)
        return [c0, c1]

    def rs_mid(i, cs):
        cs[1].wait_recv()
        rs_s2[i] = (rs_k[i, 1] + rs_r1[i, 1].astype(F32)).astype(BF)
        cs.append(send(rs_s2.at[i], rs_r2.at[i], d, ty))

    def rs_end(i, cs):
        cs[0].wait_recv()
        cs[2].wait_recv()
        return rs_k[i, 0] + rs_r1[i, 0].astype(F32) + rs_r2[i].astype(F32)

    def normalize(values):
        centre = values - jnp.mean(values, -1, keepdims=True)
        spread = lax.rsqrt(jnp.mean(centre * centre, -1, keepdims=True) + epsilon)
        return centre * spread, spread

    def left(i, a):
        t = a[...].T
        at[i] = t.reshape(groups // 2, 2, shard, rows)
        return send(at.at[i, :, 1 - bit[0]], lr.at[i], partner[0], me)

    def right(r):
        return send(r.at[0], r.at[1], partner[0], me)

    def piece(p, i, r, cr):
        cr.wait_recv()
        keep = pieces[p][0]
        m = groups // 2
        mine = at[i, :, bit[0]].reshape(m * shard, rows)
        theirs = lr[i].reshape(m * shard, rows)
        for j in range(r.shape[2] // width):
            c = slice(j * width, (j + 1) * width)
            acc = dot(mine, r[0, :, c]) + dot(theirs, r[1, :, c])
            keep[:, :, :, c] = acc.reshape(m // 2, 2, shard, width)
        return halve(p, 1)

    def keep_left(s, kind, a):
        m = groups // 4
        mine = 2 * bit[1] + bit[0]
        if shard % 128 == 0:
            for i in range(m):
                at_c = pl.ds(pl.multiple_of((4 * i + mine) * shard, shard), shard)
                atm[s, kind, i] = a[:, at_c].T
        else:
            at_tmp[...] = a[...].T.reshape(m, 4, shard, rows)
            atm[s, kind] = at_tmp[:, mine]

    def mlp_piece(p, kind, r):
        keep = pieces[p][0]
        m = groups // 4
        for j in range(hid // tile):
            c = slice(j * tile, (j + 1) * tile)
            acc = dot(atm[0, kind].reshape(m * shard, rows), r[0, :, c])
            for s in range(1, 4):
                acc = acc + dot(atm[s, kind].reshape(m * shard, rows), r[s, :, c])
            keep[:, :, :, c] = acc.reshape(m // 2, 2, shard, tile)
        return halve(p, 2)

    def bufs(p, k):
        at_k = 3 * (k - (2 if p < 2 else 1))
        return pieces[p][at_k : at_k + 3]

    def halve(p, k):
        keep, s, r = bufs(p, k)
        s[...] = keep[:, 1 - bit[k]].astype(BF)
        return send(s, r, partner[k], me)

    def merge(p, k, c):
        c.wait_recv()
        keep, s, r = bufs(p, k)
        total = keep[:, bit[k]] + r[...].astype(F32)
        if k == bits - 1:
            outs[p][...] = total[0]
            return None
        nxt = bufs(p, k + 1)[0]
        nxt[...] = total.reshape(nxt.shape)
        return halve(p, k + 1)

    outs = [o_outer, o_inner, o_qkv.at[0], o_qkv.at[1], o_qkv.at[2], o_proj]

    def gelu_parts(h):
        k0, k1 = 0.7978845608028654, 0.044715
        sq = h * h
        t = jnp.tanh(k0 * h * (1.0 + k1 * sq))
        active = (0.5 * h * (1.0 + t)).astype(BF)
        return active, 0.5 * (1.0 + t) + 0.5 * h * (1.0 - t * t) * (k0 * (1.0 + 3.0 * k1 * sq))

    def mlp_image(s):
        normed, _ = normalize(g_in[s, 0].astype(F32))
        a_more[...] = (normed * gain_mlp[...]).astype(BF)
        for j in range(hid // tile):
            c = slice(j * tile, (j + 1) * tile)
            h = dot(a_more[...], w_inner[:, c]) + bias[:, c]
            active, slope = gelu_parts(h)
            r_act[s, :, c] = active
            r_gh[s, :, c] = (dot(g_in[s, 1], w_outer[:, c]) * slope).astype(BF)
        keep_left(s, 0, a_more)
        keep_left(s, 1, g_in.at[s, 1])

    c_of = ag_start(g_of)
    c_low = ag_start(g_low)
    own = g_in.at[0, :, :, cols(me)]
    swap = [None] + [
        send(own, g_in.at[s, :, :, cols(me)], q, me)
        for s, q in ((1, partner[0]), (2, partner[1]), (3, both))
    ]
    ag_mid(g_of, c_of)
    ag_end(c_of)
    normed, sp_mlp = normalize(g_of[...].astype(F32))
    n_mlp[...] = normed
    a_mlp[...] = (normed * gain_mlp[...]).astype(BF)
    ag_mid(g_low, c_low)

    def more_start(s):
        swap[s].wait_recv()
        return ag_start(g_in.at[s])

    weights[0].wait()
    for j in range(hid // tile):
        c = slice(j * tile, (j + 1) * tile)
        h = dot(a_mlp[...], w_inner[:, c]) + bias[:, c]
        r_act[0, :, c], dgelu[:, c] = gelu_parts(h)
    ag_end(c_low)
    weights[1].wait()
    c_mlp = rs_start(0, lambda i: dot(r_act[0], w_outer[cols(i), :], NT))
    c_gf = ag_start(g_gf)
    c_1 = more_start(1)
    for j in range(hid // tile):
        c = slice(j * tile, (j + 1) * tile)
        gl = (dot(g_low[...], w_outer[:, c]) * dgelu[:, c]).astype(BF)
        r_gh[0, :, c] = gl
        sm_s[0, :, 2 * width + j * tile : 2 * width + (j + 1) * tile] = jnp.sum(
            gl.astype(F32), 0, keepdims=True
        )
    rs_mid(0, c_mlp)
    c_gn = rs_start(1, lambda i: dot(r_gh[0], w_inner[cols(i), :], NT))
    ag_mid(g_gf, c_gf)
    ag_mid(g_in.at[1], c_1)
    total = rs_end(0, c_mlp)
    second = (os_ref[0].astype(F32) - total[0:length]).astype(BF)
    o_is[0] = second
    g_is[:, cols(me)] = jnp.zeros((rows, width), BF)
    g_is[0:length, cols(me)] = second
    c_is = ag_start(g_is)
    rs_mid(1, c_gn)
    c_2 = more_start(2)
    keep_left(0, 0, a_mlp)
    keep_left(0, 1, g_low)
    ag_mid(g_is, c_is)
    total = rs_end(1, c_gn)
    g_gn[:, cols(me)] = total.astype(BF)
    c_ggn = ag_start(g_gn)
    sm_s[0, :, width : 2 * width] = jnp.sum(total * n_mlp[:, cols(me)], 0, keepdims=True)
    ag_mid(g_in.at[2], c_2)
    ag_end(c_1)
    mlp_image(1)
    ag_mid(g_gn, c_ggn)
    c_3 = more_start(3)
    ag_end(c_is)
    normed, spread = normalize(g_is[...].astype(F32))
    n_attn[...] = normed
    sp_attn[...] = jnp.broadcast_to(spread, sp_attn.shape)
    a_attn[...] = (normed * gain_attn[...]).astype(BF)
    x_attn = left(0, a_attn)
    weights[2].wait()
    for j in range(3):
        c = slice(j * width, (j + 1) * width)
        qkv[:, c] = dot(a_attn[...], w_qkv[j]).astype(BF)
    ag_end(c_gf)
    ag_end(c_ggn)

    def means(g, n, gain):
        scaled = g * gain
        return (
            jnp.mean(scaled, -1, keepdims=True),
            jnp.mean(scaled * n, -1, keepdims=True),
        )

    g = g_gn[...].astype(F32)
    first, other = means(g, n_mlp[...], gain_mlp[...])
    back = sp_mlp * (g * gain_mlp[...] - first - n_mlp[...] * other)
    a_back[...] = (g_gf[...].astype(F32) + back).astype(BF)
    o_bf[0] = a_back[0:length, cols(me)]
    weights[3].wait()
    gheads[...] = dot(a_back[...], w_proj[...]).astype(BF)
    x_back = left(1, a_back)
    ag_mid(g_in.at[3], c_3)
    ag_end(c_2)
    mlp_image(2)

    factor = HEAD**-0.5
    valid = lax.broadcasted_iota(jnp.int32, (rows, rows), 1) < length
    for h in range(width // HEAD):
        c = slice(h * HEAD, (h + 1) * HEAD)
        q = qkv[:, c]
        k = qkv[:, width + h * HEAD : width + (h + 1) * HEAD]
        v = qkv[:, 2 * width + h * HEAD : 2 * width + (h + 1) * HEAD]
        gh = gheads[:, c]
        s = jnp.where(valid, dot(q, k, NT) * factor, -1e30)
        e = jnp.exp(s - jnp.max(s, -1, keepdims=True))
        p = e / jnp.sum(e, -1, keepdims=True)
        low = p.astype(BF)
        r_attn[0, :, c] = dot(low, v).astype(BF)
        gp = dot(gh, v, NT)
        gs = (p * (gp - jnp.sum(gp * p, -1, keepdims=True))).astype(BF)
        r_rows[0, 0, :, c] = (dot(gs, k) * factor).astype(BF)
        r_rows[1, 0, :, c] = (dot(gs, q, TN) * factor).astype(BF)
        r_rows[2, 0, :, c] = dot(low, gh, TN).astype(BF)
    x_r = [right(r_rows.at[2]), right(r_rows.at[1]), right(r_rows.at[0])][::-1]
    x_attn_rows = right(r_attn)
    c_gna = rs_start(
        3,
        lambda i: dot(r_rows[0, 0], w_qkv[0, cols(i), :], NT)
        + dot(r_rows[1, 0], w_qkv[1, cols(i), :], NT)
        + dot(r_rows[2, 0], w_qkv[2, cols(i), :], NT),
    )
    c_out = rs_start(2, lambda i: dot(r_attn[0], w_proj[cols(i), :], NT))
    zs = [None] * 6
    ag_end(c_3)
    mlp_image(3)
    rs_mid(3, c_gna)
    rs_mid(2, c_out)
    zs[0] = mlp_piece(0, 1, r_act)
    x_attn.wait_recv()
    for p in (4, 3, 2):
        zs[p] = piece(p, 0, r_rows.at[p - 2], x_r[p - 2])
    x_back.wait_recv()
    zs[5] = piece(5, 1, r_attn, x_attn_rows)
    zs[1] = mlp_piece(1, 0, r_gh)
    total = rs_end(3, c_gna)
    g_gna[:, cols(me)] = total.astype(BF)
    c_ggna = ag_start(g_gna)
    sm_s[0, :, 0:width] = jnp.sum(total * n_attn[:, cols(me)], 0, keepdims=True)
    c_sm = send(sm_s.at[0], sm_r.at[0], partner[0], me)
    for p in (4, 3, 2, 5):
        zs[p] = merge(p, 1, zs[p])
    total = rs_end(2, c_out)
    o_if[0] = (of_ref[0].astype(F32) - total[0:length]).astype(BF)
    ag_mid(g_gna, c_ggna)
    c_sm.wait_recv()
    sm_s[1] = sm_s[0] + sm_r[0]
    c_sm = send(sm_s.at[1], sm_r.at[1], partner[1], me)
    ag_end(c_ggna)
    first, other = means(g_gna[...].astype(F32), n_attn[...], gain_attn[...])
    back = sp_attn[:, 0:1] * (
        g_gna[:, cols(me)].astype(F32) * gain_attn[:, cols(me)]
        - first
        - n_attn[:, cols(me)] * other
    )
    o_bs[0] = (gs_ref[0].astype(F32) + back[0:length]).astype(BF)
    for k in range(2, bits):
        c_sm.wait_recv()
        sm_s[k] = sm_s[k - 1] + sm_r[k - 1]
        c_sm = send(sm_s.at[k], sm_r.at[k], partner[k], me)
        for p in (0, 4, 3, 2, 5, 1):
            zs[p] = merge(p, k, zs[p])
    c_sm.wait_recv()
    small = sm_s[bits - 1] + sm_r[bits - 1]
    o_ga[...] = small[:, 0:width]
    o_gm[...] = small[:, width : 2 * width]
    o_bias[...] = small[:, 2 * width :]
    for c in pending:
        c.wait_send()


def on_device(
    out_first, out_second, grad_first, grad_second, gain_attn, gain_mlp,
    qkv_weight, proj_weight, inner_weight, inner_bias, outer_weight,
):
    images, length, width = out_first.shape
    parts = lax.axis_size("tensor")
    groups = lax.axis_size("dp")
    full = width * parts
    hid = inner_weight.shape[1]
    rows = (length + 15) // 16 * 16
    shard = full // groups
    bits = groups.bit_length() - 1
    sizes = (groups, length, width, full, hid, 256, rows)
    vm = pltpu.VMEM
    half = groups // 2
    scratch = [
        vm((3, full, width), BF), vm((full, width), BF), vm((full, hid), BF), vm((full, hid), BF),
    ]
    scratch += [vm((4, 2, rows, full), BF)] + [vm((rows, full), BF)] * 4
    scratch += [vm((rows, full), BF)] * 4
    scratch += [vm((rows, full), F32)] * 2 + [vm((rows, 128), F32)]
    scratch += [vm((rows, hid), F32), vm((rows, 3 * width), BF), vm((rows, width), BF)]
    scratch += [vm((2, half, 2, shard, rows), BF), vm((2, half, shard, rows), BF)]
    quarter = groups // 4
    scratch += [vm((4, 2, quarter, shard, rows), BF), vm((quarter, 4, shard, rows), BF)]
    scratch += [vm((4, rows, hid), BF), vm((4, rows, hid), BF), vm((2, rows, width), BF), vm((3, 2, rows, width), BF)]
    scratch += [
        vm((4, 2, rows, width), BF), vm((4, 2, rows, width), BF), vm((4, 2, rows, width), F32),
        vm((4, rows, width), BF), vm((4, rows, width), BF),
    ]
    small = 2 * width + hid
    scratch += [vm((bits, 1, small), F32), vm((bits, 1, small), F32)]
    for n in (hid, hid, width, width, width, width):
        m = quarter if n == hid else half
        bufs = []
        for k in range(m.bit_length() - 1):
            bufs += [vm((m // 2, 2, shard, n), F32), vm((m // 2, shard, n), BF), vm((m // 2, shard, n), BF)]
            m //= 2
        scratch.append(bufs)
    scratch += [pltpu.SemaphoreType.DMA((80,)), pltpu.SemaphoreType.DMA((80,)), pltpu.SemaphoreType.DMA((4,))]
    local = jax.ShapeDtypeStruct((images, length, width), BF)
    out_shape = [
        local, local, local, local,
        jax.ShapeDtypeStruct((3, shard, width), F32),
        jax.ShapeDtypeStruct((shard, width), F32),
        jax.ShapeDtypeStruct((shard, hid), F32),
        jax.ShapeDtypeStruct((1, width), F32),
        jax.ShapeDtypeStruct((1, width), F32),
        jax.ShapeDtypeStruct((1, hid), F32),
        jax.ShapeDtypeStruct((shard, hid), F32),
    ]
    v = pl.BlockSpec(memory_space=pltpu.VMEM)
    a = pl.BlockSpec(memory_space=pl.ANY)
    o = pl.pallas_call(
        functools.partial(kernel, sizes),
        out_shape=out_shape,
        in_specs=[v] * 7 + [a] * 4,
        out_specs=[v] * 11,
        scratch_shapes=scratch,
        compiler_params=pltpu.CompilerParams(
            collective_id=0, has_side_effects=True, vmem_limit_bytes=60 * 2**20
        ),
    )(
        out_first, out_second, grad_first, grad_second,
        gain_attn.reshape(1, full), gain_mlp.reshape(1, full), inner_bias.reshape(1, hid),
        jnp.transpose(qkv_weight, (1, 0, 2)), proj_weight, inner_weight, outer_weight,
    )
    return (
        o[0], o[1], o[2], o[3], jnp.transpose(o[4], (1, 0, 2)), o[5], o[6],
        o[9].reshape(hid), o[10], o[7].reshape(width), o[8].reshape(width),
    )


def solution(mesh):
    act = P("dp", None, "tensor")
    in_specs = (
        act, act, act, act, P(), P(), P(None, None, "tensor"), P(None, "tensor"),
        P(None, "tensor"), P("tensor"), P(None, "tensor"),
    )
    out_specs = (
        act, act, act, act, P("dp", None, "tensor"), P("dp", "tensor"), P("dp", "tensor"),
        P("tensor"), P("dp", "tensor"), P("tensor"), P("tensor"),
    )
    return jax.shard_map(
        on_device, mesh=mesh, in_specs=in_specs, out_specs=out_specs, check_vma=False
    )
```

```python
import functools

import jax
import jax.numpy as jnp
from jax import lax
from jax.experimental import pallas as pl
from jax.experimental.pallas import tpu as pltpu
from jax.sharding import PartitionSpec as P

epsilon = 1e-06
HEAD = 64
BF = jnp.bfloat16
F32 = jnp.float32
MESH = pl.DeviceIdType.MESH
LIMIT = 61 * 2**20


def dot(a, b, dims=((1,), (0,))):
    return lax.dot_general(a, b, (dims, ((), ())), preferred_element_type=F32)


NT = ((1,), (1,))
TN = ((0,), (0,))


def kernel(
    sizes,
    of_ref, os_ref, gf_ref, gs_ref, gain_attn, gain_mlp, bias,
    qkv_hbm, proj_hbm, inner_hbm, outer_hbm,
    o_if, o_is, o_bf, o_bs, o_qkv, o_proj, o_inner, o_ga, o_gm, o_bias, o_outer,
    w_qkv, w_proj, w_inner, w_outer,
    g_in, g_gf, g_is, g_gn, g_gna,
    a_mlp, a_more, a_attn, a_back, n_mlp, n_attn, sp_attn,
    dgelu, qkv, gheads,
    at, lr, atm, at_tmp,
    r_act, r_gh, r_attn, r_rows,
    rs_s1, rs_r1, rs_k, rs_s2, rs_r2,
    sm_s, sm_r,
    *rest,
):
    groups, length, width, full, hid, tile, rows = sizes
    bits = groups.bit_length() - 1
    shard = full // groups
    pieces = rest[:-3]
    ssem, rsem, wsem = rest[-3:]
    d = lax.axis_index("dp")
    me = lax.axis_index("tensor")
    core, yy = me % 2, me // 2
    tc = yy * 2 + 1 - core
    ty = (1 - yy) * 2 + core
    td = (1 - yy) * 2 + 1 - core
    bit = [(d // 2**k) % 2 for k in range(bits)]
    partner = [d + (1 - 2 * bit[k]) * 2**k for k in range(bits)]
    counter = [0]
    pending = []

    def send(src, dst, dp_id, t_id):
        k = counter[0]
        counter[0] += 1
        c = pltpu.make_async_remote_copy(
            src_ref=src, dst_ref=dst, send_sem=ssem.at[k], recv_sem=rsem.at[k],
            device_id=(dp_id, t_id), device_id_type=MESH,
        )
        c.start()
        pending.append(c)
        return c

    def cols(i):
        return pl.ds(pl.multiple_of(i * width, width), width)

    weights = []
    for i, (src, dst) in enumerate(
        [(inner_hbm, w_inner), (outer_hbm, w_outer), (qkv_hbm, w_qkv), (proj_hbm, w_proj)]
    ):
        c = pltpu.make_async_copy(src, dst, wsem.at[i])
        c.start()
        weights.append(c)

    barrier = pltpu.get_barrier_semaphore()
    peers = [(d, tc), (d, ty)] + [(p, me) for p in partner]
    for peer in peers:
        pl.semaphore_signal(barrier, inc=1, device_id=peer, device_id_type=MESH)

    def stage(g, src):
        g[:, cols(me)] = jnp.zeros((rows, width), BF)
        g[0:length, cols(me)] = src[0]

    g_of, g_low = g_in.at[0, 0], g_in.at[0, 1]
    stage(g_of, of_ref)
    stage(g_low, gs_ref)
    stage(g_gf, gf_ref)
    pl.semaphore_wait(barrier, len(peers))

    def part_of(g, i):
        return g.at[:, cols(i)] if len(g.shape) == 2 else g.at[:, :, cols(i)]

    def ag_start(g):
        own = part_of(g, me)
        c2 = send(own, own, d, ty)
        c1 = send(own, own, d, tc)
        return [c1, c2]

    def ag_mid(g, cs):
        cs[1].wait_recv()
        far = part_of(g, ty)
        cs.append(send(far, far, d, tc))

    def ag_end(cs):
        cs[0].wait_recv()
        cs[2].wait_recv()

    def rs_start(i, part):
        rs_s1[i, 0] = part(tc).astype(BF)
        c0 = send(rs_s1.at[i, 0], rs_r1.at[i, 0], d, tc)
        rs_s1[i, 1] = part(td).astype(BF)
        c1 = send(rs_s1.at[i, 1], rs_r1.at[i, 1], d, tc)
        rs_k[i, 1] = part(ty)
        rs_k[i, 0] = part(me)
        return [c0, c1]

    def rs_mid(i, cs):
        cs[1].wait_recv()
        rs_s2[i] = (rs_k[i, 1] + rs_r1[i, 1].astype(F32)).astype(BF)
        cs.append(send(rs_s2.at[i], rs_r2.at[i], d, ty))

    def rs_end(i, cs):
        cs[0].wait_recv()
        cs[2].wait_recv()
        return rs_k[i, 0] + rs_r1[i, 0].astype(F32) + rs_r2[i].astype(F32)

    def normalize(values):
        centre = values - jnp.mean(values, -1, keepdims=True)
        spread = lax.rsqrt(jnp.mean(centre * centre, -1, keepdims=True) + epsilon)
        return centre * spread, spread

    def left(i, a):
        t = a[...].T
        at[i] = t.reshape(groups // 2, 2, shard, rows)
        return send(at.at[i, :, 1 - bit[0]], lr.at[i], partner[0], me)

    def right(r):
        return send(r.at[0], r.at[1], partner[0], me)

    def piece(p, i, r, cr):
        cr.wait_recv()
        keep = pieces[p][0]
        m = groups // 2
        mine = at[i, :, bit[0]].reshape(m * shard, rows)
        theirs = lr[i].reshape(m * shard, rows)
        for j in range(r.shape[2] // width):
            c = slice(j * width, (j + 1) * width)
            acc = dot(mine, r[0, :, c]) + dot(theirs, r[1, :, c])
            keep[:, :, :, c] = acc.reshape(m // 2, 2, shard, width)
        return halve(p, 1)

    def keep_left(s, kind, a):
        m = groups // 2
        if shard % 128 == 0:
            for i in range(m):
                at_c = pl.ds(pl.multiple_of((2 * i + bit[0]) * shard, shard), shard)
                atm[s, kind, i] = a[:, at_c].T
        else:
            at_tmp[...] = a[...].T.reshape(m, 2, shard, rows)
            atm[s, kind] = at_tmp[:, bit[0]]

    def mlp_piece(p, kind, r):
        keep = pieces[p][0]
        m = groups // 2
        for j in range(hid // tile):
            c = slice(j * tile, (j + 1) * tile)
            acc = dot(atm[0, kind].reshape(m * shard, rows), r[0, :, c])
            for s in range(1, 2):
                acc = acc + dot(atm[s, kind].reshape(m * shard, rows), r[s, :, c])
            keep[:, :, :, c] = acc.reshape(m // 2, 2, shard, tile)
        return halve(p, 1)

    def bufs(p, k):
        at_k = 3 * (k - 1)
        return pieces[p][at_k : at_k + 3]

    def halve(p, k):
        keep, s, r = bufs(p, k)
        s[...] = keep[:, 1 - bit[k]].astype(BF)
        return send(s, r, partner[k], me)

    def merge(p, k, c):
        c.wait_recv()
        keep, s, r = bufs(p, k)
        total = keep[:, bit[k]] + r[...].astype(F32)
        if k == bits - 1:
            outs[p][...] = total[0]
            return None
        nxt = bufs(p, k + 1)[0]
        nxt[...] = total.reshape(nxt.shape)
        return halve(p, k + 1)

    outs = [o_outer, o_inner, o_qkv.at[0], o_qkv.at[1], o_qkv.at[2], o_proj]

    def gelu_parts(h):
        k0, k1 = 0.7978845608028654, 0.044715
        sq = h * h
        t = jnp.tanh(k0 * h * (1.0 + k1 * sq))
        active = (0.5 * h * (1.0 + t)).astype(BF)
        return active, 0.5 * (1.0 + t) + 0.5 * h * (1.0 - t * t) * (k0 * (1.0 + 3.0 * k1 * sq))

    def image_active():
        normed, _ = normalize(g_in[1, 0].astype(F32))
        a_more[...] = (normed * gain_mlp[...]).astype(BF)
        for j in range(hid // tile):
            c = slice(j * tile, (j + 1) * tile)
            h = dot(a_more[...], w_inner[:, c]) + bias[:, c]
            r_act[1, :, c], dgelu[:, c] = gelu_parts(h)

    def image_grad():
        for j in range(hid // tile):
            c = slice(j * tile, (j + 1) * tile)
            r_gh[1, :, c] = (dot(g_in[1, 1], w_outer[:, c]) * dgelu[:, c]).astype(BF)

    c_of = ag_start(g_of)
    c_low = ag_start(g_low)
    own = g_in.at[0, :, :, cols(me)]
    swap = send(own, g_in.at[1, :, :, cols(me)], partner[0], me)
    ag_mid(g_of, c_of)
    ag_end(c_of)
    normed, sp_mlp = normalize(g_of[...].astype(F32))
    n_mlp[...] = normed
    a_mlp[...] = (normed * gain_mlp[...]).astype(BF)
    ag_mid(g_low, c_low)

    swap.wait_recv()
    c_1 = ag_start(g_in.at[1])
    weights[0].wait()
    for j in range(hid // tile):
        c = slice(j * tile, (j + 1) * tile)
        h = dot(a_mlp[...], w_inner[:, c]) + bias[:, c]
        r_act[0, :, c], dgelu[:, c] = gelu_parts(h)
    ag_end(c_low)
    weights[1].wait()
    c_mlp = rs_start(0, lambda i: dot(r_act[0], w_outer[cols(i), :], NT))
    for j in range(hid // tile):
        c = slice(j * tile, (j + 1) * tile)
        gl = (dot(g_low[...], w_outer[:, c]) * dgelu[:, c]).astype(BF)
        r_gh[0, :, c] = gl
        sm_s[0, :, 2 * width + j * tile : 2 * width + (j + 1) * tile] = jnp.sum(
            gl.astype(F32), 0, keepdims=True
        )
    rs_mid(0, c_mlp)
    c_gn = rs_start(1, lambda i: dot(r_gh[0], w_inner[cols(i), :], NT))
    ag_mid(g_in.at[1], c_1)
    ag_end(c_1)
    image_active()
    rs_mid(1, c_gn)
    total = rs_end(0, c_mlp)
    second = (os_ref[0].astype(F32) - total[0:length]).astype(BF)
    o_is[0] = second
    g_is[:, cols(me)] = jnp.zeros((rows, width), BF)
    g_is[0:length, cols(me)] = second
    c_is = ag_start(g_is)
    c_gf = ag_start(g_gf)
    keep_left(0, 1, g_low)
    keep_left(1, 1, g_in.at[1, 1])
    zs = [None] * 6
    zs[0] = mlp_piece(0, 1, r_act)
    ag_mid(g_is, c_is)
    total = rs_end(1, c_gn)
    g_gn[:, cols(me)] = total.astype(BF)
    c_ggn = ag_start(g_gn)
    sm_s[0, :, width : 2 * width] = jnp.sum(total * n_mlp[:, cols(me)], 0, keepdims=True)
    image_grad()
    ag_mid(g_gf, c_gf)
    ag_end(c_is)
    normed, spread = normalize(g_is[...].astype(F32))
    n_attn[...] = normed
    sp_attn[...] = jnp.broadcast_to(spread, sp_attn.shape)
    a_attn[...] = (normed * gain_attn[...]).astype(BF)
    x_attn = left(0, a_attn)
    ag_mid(g_gn, c_ggn)
    weights[2].wait()
    for j in range(3):
        c = slice(j * width, (j + 1) * width)
        qkv[:, c] = dot(a_attn[...], w_qkv[j]).astype(BF)
    keep_left(0, 0, a_mlp)
    keep_left(1, 0, a_more)
    zs[1] = mlp_piece(1, 0, r_gh)
    ag_end(c_gf)
    ag_end(c_ggn)

    def means(g, n, gain):
        scaled = g * gain
        return (
            jnp.mean(scaled, -1, keepdims=True),
            jnp.mean(scaled * n, -1, keepdims=True),
        )

    g = g_gn[...].astype(F32)
    first, other = means(g, n_mlp[...], gain_mlp[...])
    back = sp_mlp * (g * gain_mlp[...] - first - n_mlp[...] * other)
    a_back[...] = (g_gf[...].astype(F32) + back).astype(BF)
    o_bf[0] = a_back[0:length, cols(me)]
    weights[3].wait()
    gheads[...] = dot(a_back[...], w_proj[...]).astype(BF)
    x_back = left(1, a_back)
    zs[0] = merge(0, 1, zs[0])

    factor = HEAD**-0.5
    valid = lax.broadcasted_iota(jnp.int32, (rows, rows), 1) < length
    for h in range(width // HEAD):
        c = slice(h * HEAD, (h + 1) * HEAD)
        q = qkv[:, c]
        k = qkv[:, width + h * HEAD : width + (h + 1) * HEAD]
        v = qkv[:, 2 * width + h * HEAD : 2 * width + (h + 1) * HEAD]
        gh = gheads[:, c]
        s = jnp.where(valid, dot(q, k, NT) * factor, -1e30)
        e = jnp.exp(s - jnp.max(s, -1, keepdims=True))
        p = e / jnp.sum(e, -1, keepdims=True)
        low = p.astype(BF)
        r_attn[0, :, c] = dot(low, v).astype(BF)
        gp = dot(gh, v, NT)
        gs = (p * (gp - jnp.sum(gp * p, -1, keepdims=True))).astype(BF)
        r_rows[0, 0, :, c] = (dot(gs, k) * factor).astype(BF)
        r_rows[1, 0, :, c] = (dot(gs, q, TN) * factor).astype(BF)
        r_rows[2, 0, :, c] = dot(low, gh, TN).astype(BF)
    x_r = [right(r_rows.at[2]), right(r_rows.at[1]), right(r_rows.at[0])][::-1]
    x_attn_rows = right(r_attn)
    c_gna = rs_start(
        3,
        lambda i: dot(r_rows[0, 0], w_qkv[0, cols(i), :], NT)
        + dot(r_rows[1, 0], w_qkv[1, cols(i), :], NT)
        + dot(r_rows[2, 0], w_qkv[2, cols(i), :], NT),
    )
    c_out = rs_start(2, lambda i: dot(r_attn[0], w_proj[cols(i), :], NT))
    zs[1] = merge(1, 1, zs[1])
    rs_mid(3, c_gna)
    rs_mid(2, c_out)
    x_attn.wait_recv()
    for p in (4, 3, 2):
        zs[p] = piece(p, 0, r_rows.at[p - 2], x_r[p - 2])
    x_back.wait_recv()
    zs[5] = piece(5, 1, r_attn, x_attn_rows)
    total = rs_end(3, c_gna)
    g_gna[:, cols(me)] = total.astype(BF)
    c_ggna = ag_start(g_gna)
    sm_s[0, :, 0:width] = jnp.sum(total * n_attn[:, cols(me)], 0, keepdims=True)
    c_sm = send(sm_s.at[0], sm_r.at[0], partner[0], me)
    for p in (4, 3, 2, 5):
        zs[p] = merge(p, 1, zs[p])
    total = rs_end(2, c_out)
    o_if[0] = (of_ref[0].astype(F32) - total[0:length]).astype(BF)
    ag_mid(g_gna, c_ggna)
    c_sm.wait_recv()
    sm_s[1] = sm_s[0] + sm_r[0]
    c_sm = send(sm_s.at[1], sm_r.at[1], partner[1], me)
    ag_end(c_ggna)
    first, other = means(g_gna[...].astype(F32), n_attn[...], gain_attn[...])
    back = sp_attn[:, 0:1] * (
        g_gna[:, cols(me)].astype(F32) * gain_attn[:, cols(me)]
        - first
        - n_attn[:, cols(me)] * other
    )
    o_bs[0] = (gs_ref[0].astype(F32) + back[0:length]).astype(BF)
    for k in range(2, bits):
        c_sm.wait_recv()
        sm_s[k] = sm_s[k - 1] + sm_r[k - 1]
        c_sm = send(sm_s.at[k], sm_r.at[k], partner[k], me)
        for p in (0, 1, 4, 3, 2, 5):
            zs[p] = merge(p, k, zs[p])
    c_sm.wait_recv()
    small = sm_s[bits - 1] + sm_r[bits - 1]
    o_ga[...] = small[:, 0:width]
    o_gm[...] = small[:, width : 2 * width]
    o_bias[...] = small[:, 2 * width :]
    for c in pending:
        c.wait_send()


def hand_out(*refs):
    count = (len(refs) - 2) // 3
    source, target, held = refs[:count], refs[count : 2 * count], refs[2 * count : 3 * count]
    first = [pltpu.make_async_copy(source[i], held[i], refs[-2].at[i]) for i in range(count)]
    second = [pltpu.make_async_copy(held[i], target[i], refs[-1].at[i]) for i in range(count)]
    for c in first:
        c.start()
    for c, e in zip(first, second):
        c.wait()
        e.start()
    for e in second:
        e.wait()


def on_device(
    out_first, out_second, grad_first, grad_second, gain_attn, gain_mlp,
    qkv_weight, proj_weight, inner_weight, inner_bias, outer_weight,
):
    images, length, width = out_first.shape
    parts = lax.axis_size("tensor")
    groups = lax.axis_size("dp")
    full = width * parts
    hid = inner_weight.shape[1]
    rows = (length + 15) // 16 * 16
    shard = full // groups
    bits = groups.bit_length() - 1
    sizes = (groups, length, width, full, hid, 256, rows)
    vm = pltpu.VMEM
    half = groups // 2
    scratch = [
        vm((3, full, width), BF), vm((full, width), BF), vm((full, hid), BF), vm((full, hid), BF),
    ]
    scratch += [vm((2, 2, rows, full), BF)] + [vm((rows, full), BF)] * 4
    scratch += [vm((rows, full), BF)] * 4
    scratch += [vm((rows, full), F32)] * 2 + [vm((rows, 128), F32)]
    scratch += [vm((rows, hid), F32), vm((rows, 3 * width), BF), vm((rows, width), BF)]
    scratch += [vm((2, half, 2, shard, rows), BF), vm((2, half, shard, rows), BF)]
    scratch += [vm((2, 2, half, shard, rows), BF), vm((half, 2, shard, rows), BF)]
    scratch += [vm((2, rows, hid), BF), vm((2, rows, hid), BF), vm((2, rows, width), BF), vm((3, 2, rows, width), BF)]
    scratch += [
        vm((4, 2, rows, width), BF), vm((4, 2, rows, width), BF), vm((4, 2, rows, width), F32),
        vm((4, rows, width), BF), vm((4, rows, width), BF),
    ]
    small = 2 * width + hid
    scratch += [vm((bits, 1, small), F32), vm((bits, 1, small), F32)]
    for n in (hid, hid, width, width, width, width):
        m = half
        bufs = []
        for k in range(m.bit_length() - 1):
            bufs += [vm((m // 2, 2, shard, n), F32), vm((m // 2, shard, n), BF), vm((m // 2, shard, n), BF)]
            m //= 2
        scratch.append(bufs)
    scratch += [pltpu.SemaphoreType.DMA((80,)), pltpu.SemaphoreType.DMA((80,)), pltpu.SemaphoreType.DMA((4,))]
    local = jax.ShapeDtypeStruct((images, length, width), BF)
    out_shape = [
        local, local, local, local,
        jax.ShapeDtypeStruct((3, shard, width), F32),
        jax.ShapeDtypeStruct((shard, width), F32),
        jax.ShapeDtypeStruct((shard, hid), F32),
        jax.ShapeDtypeStruct((1, width), F32),
        jax.ShapeDtypeStruct((1, width), F32),
        jax.ShapeDtypeStruct((1, hid), F32),
        jax.ShapeDtypeStruct((shard, hid), F32),
    ]
    v = pl.BlockSpec(memory_space=pltpu.VMEM)
    a = pl.BlockSpec(memory_space=pl.ANY)
    hbm = pl.BlockSpec(memory_space=pltpu.HBM)
    o = pl.pallas_call(
        functools.partial(kernel, sizes),
        out_shape=out_shape,
        in_specs=[v] * 7 + [hbm] * 4,
        out_specs=[v] * 11,
        scratch_shapes=scratch,
        compiler_params=pltpu.CompilerParams(
            collective_id=0, has_side_effects=True, vmem_limit_bytes=LIMIT
        ),
    )(
        out_first, out_second, grad_first, grad_second,
        gain_attn.reshape(1, full), gain_mlp.reshape(1, full), inner_bias.reshape(1, hid),
        jnp.transpose(qkv_weight, (1, 0, 2)), proj_weight, inner_weight, outer_weight,
    )
    o = pl.pallas_call(
        hand_out,
        out_shape=out_shape,
        in_specs=[a] * 11,
        out_specs=[a] * 11,
        scratch_shapes=[vm(x.shape, x.dtype) for x in out_shape]
        + [pltpu.SemaphoreType.DMA((11,)), pltpu.SemaphoreType.DMA((11,))],
        compiler_params=pltpu.CompilerParams(vmem_limit_bytes=LIMIT),
    )(*o)
    return (
        o[0], o[1], o[2], o[3], jnp.transpose(o[4], (1, 0, 2)), o[5], o[6],
        o[9].reshape(hid), o[10], o[7].reshape(width), o[8].reshape(width),
    )


def solution(mesh):
    act = P("dp", None, "tensor")
    in_specs = (
        act, act, act, act, P(), P(), P(None, None, "tensor"), P(None, "tensor"),
        P(None, "tensor"), P("tensor"), P(None, "tensor"),
    )
    out_specs = (
        act, act, act, act, P("dp", None, "tensor"), P("dp", "tensor"), P("dp", "tensor"),
        P("tensor"), P("dp", "tensor"), P("tensor"), P("tensor"),
    )
    return jax.shard_map(
        on_device, mesh=mesh, in_specs=in_specs, out_specs=out_specs, check_vma=False
    )
```

```python
import functools

import jax
import jax.numpy as jnp
from jax import lax
from jax.experimental import pallas as pl
from jax.experimental.pallas import tpu as pltpu
from jax.sharding import PartitionSpec as P

epsilon = 1e-06
HEAD = 64
BF = jnp.bfloat16
F32 = jnp.float32
MESH = pl.DeviceIdType.MESH
LIMIT = 61 * 2**20


def dot(a, b, dims=((1,), (0,))):
    return lax.dot_general(a, b, (dims, ((), ())), preferred_element_type=F32)


NT = ((1,), (1,))
TN = ((0,), (0,))


def kernel(
    sizes,
    of_ref, os_ref, gf_ref, gs_ref, gain_attn, gain_mlp, bias,
    qkv_hbm, proj_hbm, inner_hbm, outer_hbm,
    o_if, o_is, o_bf, o_bs, o_qkv, o_proj, o_inner, o_ga, o_gm, o_bias, o_outer,
    w_qkv, w_proj, w_inner, w_outer,
    g_in, g_gf, g_is, g_gn, g_gna,
    a_mlp, a_more, a_attn, a_back, n_mlp, n_attn, sp_attn,
    dgelu, qkv, gheads,
    at, lr, atm, at_tmp,
    r_act, r_gh, r_attn, r_rows,
    rs_s1, rs_r1, rs_k, rs_s2, rs_r2,
    sm_s, sm_r,
    *rest,
):
    groups, length, width, full, hid, tile, rows = sizes
    bits = groups.bit_length() - 1
    shard = full // groups
    pieces = rest[:-3]
    ssem, rsem, wsem = rest[-3:]
    d = lax.axis_index("dp")
    me = lax.axis_index("tensor")
    core, yy = me % 2, me // 2
    tc = yy * 2 + 1 - core
    ty = (1 - yy) * 2 + core
    td = (1 - yy) * 2 + 1 - core
    bit = [(d // 2**k) % 2 for k in range(bits)]
    partner = [d + (1 - 2 * bit[k]) * 2**k for k in range(bits)]
    counter = [0]
    pending = []

    def send(src, dst, dp_id, t_id):
        k = counter[0]
        counter[0] += 1
        c = pltpu.make_async_remote_copy(
            src_ref=src, dst_ref=dst, send_sem=ssem.at[k], recv_sem=rsem.at[k],
            device_id=(dp_id, t_id), device_id_type=MESH,
        )
        c.start()
        pending.append(c)
        return c

    def cols(i):
        return pl.ds(pl.multiple_of(i * width, width), width)

    weights = []
    for i, (src, dst) in enumerate(
        [(inner_hbm, w_inner), (outer_hbm, w_outer), (qkv_hbm, w_qkv), (proj_hbm, w_proj)]
    ):
        c = pltpu.make_async_copy(src, dst, wsem.at[i])
        c.start()
        weights.append(c)

    barrier = pltpu.get_barrier_semaphore()
    peers = [(d, tc), (d, ty)] + [(p, me) for p in partner]
    for peer in peers:
        pl.semaphore_signal(barrier, inc=1, device_id=peer, device_id_type=MESH)

    def stage(g, src):
        g[:, cols(me)] = jnp.zeros((rows, width), BF)
        g[0:length, cols(me)] = src[0]

    g_of, g_low = g_in.at[0, 0], g_in.at[0, 1]
    stage(g_of, of_ref)
    stage(g_low, gs_ref)
    stage(g_gf, gf_ref)
    pl.semaphore_wait(barrier, len(peers))

    def part_of(g, i):
        return g.at[:, cols(i)] if len(g.shape) == 2 else g.at[:, :, cols(i)]

    def ag_start(g):
        own = part_of(g, me)
        c2 = send(own, own, d, ty)
        c1 = send(own, own, d, tc)
        return [c1, c2]

    def ag_mid(g, cs):
        cs[1].wait_recv()
        far = part_of(g, ty)
        cs.append(send(far, far, d, tc))

    def ag_end(cs):
        cs[0].wait_recv()
        cs[2].wait_recv()

    def rs_start(i, part):
        rs_s1[i, 0] = part(tc).astype(BF)
        c0 = send(rs_s1.at[i, 0], rs_r1.at[i, 0], d, tc)
        rs_s1[i, 1] = part(td).astype(BF)
        c1 = send(rs_s1.at[i, 1], rs_r1.at[i, 1], d, tc)
        rs_k[i, 1] = part(ty)
        rs_k[i, 0] = part(me)
        return [c0, c1]

    def rs_mid(i, cs):
        cs[1].wait_recv()
        rs_s2[i] = (rs_k[i, 1] + rs_r1[i, 1].astype(F32)).astype(BF)
        cs.append(send(rs_s2.at[i], rs_r2.at[i], d, ty))

    def rs_end(i, cs):
        cs[0].wait_recv()
        cs[2].wait_recv()
        return rs_k[i, 0] + rs_r1[i, 0].astype(F32) + rs_r2[i].astype(F32)

    def normalize(values):
        centre = values - jnp.mean(values, -1, keepdims=True)
        spread = lax.rsqrt(jnp.mean(centre * centre, -1, keepdims=True) + epsilon)
        return centre * spread, spread

    def left(i, a):
        t = a[...].T
        at[i] = t.reshape(groups // 2, 2, shard, rows)
        return send(at.at[i, :, 1 - bit[0]], lr.at[i], partner[0], me)

    def right(r):
        return send(r.at[0], r.at[1], partner[0], me)

    def piece(p, i, r, cr):
        cr.wait_recv()
        keep = pieces[p][0]
        m = groups // 2
        mine = at[i, :, bit[0]].reshape(m * shard, rows)
        theirs = lr[i].reshape(m * shard, rows)
        for j in range(r.shape[2] // width):
            c = slice(j * width, (j + 1) * width)
            acc = dot(mine, r[0, :, c]) + dot(theirs, r[1, :, c])
            keep[:, :, :, c] = acc.reshape(m // 2, 2, shard, width)
        return halve(p, 1)

    def keep_left(s, kind, a):
        m = groups // 2
        if shard % 128 == 0:
            for i in range(m):
                at_c = pl.ds(pl.multiple_of((2 * i + bit[0]) * shard, shard), shard)
                atm[s, kind, i] = a[:, at_c].T
        else:
            at_tmp[...] = a[...].T.reshape(m, 2, shard, rows)
            atm[s, kind] = at_tmp[:, bit[0]]

    def mlp_piece(p, kind, r):
        keep = pieces[p][0]
        m = groups // 2
        for j in range(hid // tile):
            c = slice(j * tile, (j + 1) * tile)
            acc = dot(atm[0, kind].reshape(m * shard, rows), r[0, :, c])
            for s in range(1, 2):
                acc = acc + dot(atm[s, kind].reshape(m * shard, rows), r[s, :, c])
            keep[:, :, :, c] = acc.reshape(m // 2, 2, shard, tile)
        return halve(p, 1)

    def bufs(p, k):
        at_k = 3 * (k - 1)
        return pieces[p][at_k : at_k + 3]

    def halve(p, k):
        keep, s, r = bufs(p, k)
        s[...] = keep[:, 1 - bit[k]].astype(BF)
        return send(s, r, partner[k], me)

    def merge(p, k, c):
        c.wait_recv()
        keep, s, r = bufs(p, k)
        total = keep[:, bit[k]] + r[...].astype(F32)
        if k == bits - 1:
            outs[p][...] = total[0]
            return None
        nxt = bufs(p, k + 1)[0]
        nxt[...] = total.reshape(nxt.shape)
        return halve(p, k + 1)

    outs = [o_outer, o_inner, o_qkv.at[0], o_qkv.at[1], o_qkv.at[2], o_proj]

    def gelu_parts(h):
        k0, k1 = 0.7978845608028654, 0.044715
        sq = h * h
        t = jnp.tanh(k0 * h * (1.0 + k1 * sq))
        active = (0.5 * h * (1.0 + t)).astype(BF)
        return active, 0.5 * (1.0 + t) + 0.5 * h * (1.0 - t * t) * (k0 * (1.0 + 3.0 * k1 * sq))

    def image_active():
        normed, _ = normalize(g_in[1, 0].astype(F32))
        a_more[...] = (normed * gain_mlp[...]).astype(BF)
        for j in range(hid // tile):
            c = slice(j * tile, (j + 1) * tile)
            h = dot(a_more[...], w_inner[:, c]) + bias[:, c]
            r_act[1, :, c], dgelu[:, c] = gelu_parts(h)

    def image_grad():
        for j in range(hid // tile):
            c = slice(j * tile, (j + 1) * tile)
            r_gh[1, :, c] = (dot(g_in[1, 1], w_outer[:, c]) * dgelu[:, c]).astype(BF)

    c_of = ag_start(g_of)
    c_low = ag_start(g_low)
    own = g_in.at[0, :, :, cols(me)]
    swap = send(own, g_in.at[1, :, :, cols(me)], partner[0], me)
    ag_mid(g_of, c_of)
    ag_end(c_of)
    normed, sp_mlp = normalize(g_of[...].astype(F32))
    n_mlp[...] = normed
    a_mlp[...] = (normed * gain_mlp[...]).astype(BF)
    ag_mid(g_low, c_low)

    swap.wait_recv()
    c_1 = ag_start(g_in.at[1])
    weights[0].wait()
    for j in range(hid // tile):
        c = slice(j * tile, (j + 1) * tile)
        h = dot(a_mlp[...], w_inner[:, c]) + bias[:, c]
        r_act[0, :, c], dgelu[:, c] = gelu_parts(h)
    ag_end(c_low)
    weights[1].wait()
    c_mlp = rs_start(0, lambda i: dot(r_act[0], w_outer[cols(i), :], NT))
    for j in range(hid // tile):
        c = slice(j * tile, (j + 1) * tile)
        gl = (dot(g_low[...], w_outer[:, c]) * dgelu[:, c]).astype(BF)
        r_gh[0, :, c] = gl
        sm_s[0, :, 2 * width + j * tile : 2 * width + (j + 1) * tile] = jnp.sum(
            gl.astype(F32), 0, keepdims=True
        )
    rs_mid(0, c_mlp)
    c_gn = rs_start(1, lambda i: dot(r_gh[0], w_inner[cols(i), :], NT))
    ag_mid(g_in.at[1], c_1)
    ag_end(c_1)
    image_active()
    rs_mid(1, c_gn)
    total = rs_end(0, c_mlp)
    second = (os_ref[0].astype(F32) - total[0:length]).astype(BF)
    o_is[0] = second
    g_is[:, cols(me)] = jnp.zeros((rows, width), BF)
    g_is[0:length, cols(me)] = second
    c_is = ag_start(g_is)
    c_gf = ag_start(g_gf)
    keep_left(0, 1, g_low)
    keep_left(1, 1, g_in.at[1, 1])
    zs = [None] * 6
    zs[0] = mlp_piece(0, 1, r_act)
    ag_mid(g_is, c_is)
    total = rs_end(1, c_gn)
    g_gn[:, cols(me)] = total.astype(BF)
    c_ggn = ag_start(g_gn)
    sm_s[0, :, width : 2 * width] = jnp.sum(total * n_mlp[:, cols(me)], 0, keepdims=True)
    image_grad()
    ag_mid(g_gf, c_gf)
    ag_end(c_is)
    normed, spread = normalize(g_is[...].astype(F32))
    n_attn[...] = normed
    sp_attn[...] = jnp.broadcast_to(spread, sp_attn.shape)
    a_attn[...] = (normed * gain_attn[...]).astype(BF)
    x_attn = left(0, a_attn)
    ag_mid(g_gn, c_ggn)
    weights[2].wait()
    for j in range(3):
        c = slice(j * width, (j + 1) * width)
        qkv[:, c] = dot(a_attn[...], w_qkv[j]).astype(BF)
    keep_left(0, 0, a_mlp)
    keep_left(1, 0, a_more)
    zs[1] = mlp_piece(1, 0, r_gh)
    ag_end(c_gf)
    ag_end(c_ggn)

    def means(g, n, gain):
        scaled = g * gain
        return (
            jnp.mean(scaled, -1, keepdims=True),
            jnp.mean(scaled * n, -1, keepdims=True),
        )

    g = g_gn[...].astype(F32)
    first, other = means(g, n_mlp[...], gain_mlp[...])
    back = sp_mlp * (g * gain_mlp[...] - first - n_mlp[...] * other)
    a_back[...] = (g_gf[...].astype(F32) + back).astype(BF)
    o_bf[0] = a_back[0:length, cols(me)]
    weights[3].wait()
    gheads[...] = dot(a_back[...], w_proj[...]).astype(BF)
    x_back = left(1, a_back)
    zs[0] = merge(0, 1, zs[0])

    factor = HEAD**-0.5
    valid = lax.broadcasted_iota(jnp.int32, (rows, rows), 1) < length
    for h in range(width // HEAD):
        c = slice(h * HEAD, (h + 1) * HEAD)
        q = qkv[:, c]
        k = qkv[:, width + h * HEAD : width + (h + 1) * HEAD]
        v = qkv[:, 2 * width + h * HEAD : 2 * width + (h + 1) * HEAD]
        gh = gheads[:, c]
        s = jnp.where(valid, dot(q, k, NT) * factor, -1e30)
        e = jnp.exp(s - jnp.max(s, -1, keepdims=True))
        p = e / jnp.sum(e, -1, keepdims=True)
        low = p.astype(BF)
        r_attn[0, :, c] = dot(low, v).astype(BF)
        gp = dot(gh, v, NT)
        gs = (p * (gp - jnp.sum(gp * p, -1, keepdims=True))).astype(BF)
        r_rows[0, 0, :, c] = (dot(gs, k) * factor).astype(BF)
        r_rows[1, 0, :, c] = (dot(gs, q, TN) * factor).astype(BF)
        r_rows[2, 0, :, c] = dot(low, gh, TN).astype(BF)
    x_r = [right(r_rows.at[2]), right(r_rows.at[1]), right(r_rows.at[0])][::-1]
    x_attn_rows = right(r_attn)
    c_gna = rs_start(
        3,
        lambda i: dot(r_rows[0, 0], w_qkv[0, cols(i), :], NT)
        + dot(r_rows[1, 0], w_qkv[1, cols(i), :], NT)
        + dot(r_rows[2, 0], w_qkv[2, cols(i), :], NT),
    )
    c_out = rs_start(2, lambda i: dot(r_attn[0], w_proj[cols(i), :], NT))
    rs_mid(3, c_gna)
    rs_mid(2, c_out)
    x_attn.wait_recv()
    for p in (4, 3, 2):
        zs[p] = piece(p, 0, r_rows.at[p - 2], x_r[p - 2])
    x_back.wait_recv()
    zs[5] = piece(5, 1, r_attn, x_attn_rows)
    zs[1] = merge(1, 1, zs[1])
    total = rs_end(3, c_gna)
    g_gna[:, cols(me)] = total.astype(BF)
    c_ggna = ag_start(g_gna)
    sm_s[0, :, 0:width] = jnp.sum(total * n_attn[:, cols(me)], 0, keepdims=True)
    c_sm = send(sm_s.at[0], sm_r.at[0], partner[0], me)
    for p in (4, 3, 2, 5):
        zs[p] = merge(p, 1, zs[p])
    total = rs_end(2, c_out)
    o_if[0] = (of_ref[0].astype(F32) - total[0:length]).astype(BF)
    ag_mid(g_gna, c_ggna)
    c_sm.wait_recv()
    sm_s[1] = sm_s[0] + sm_r[0]
    c_sm = send(sm_s.at[1], sm_r.at[1], partner[1], me)
    ag_end(c_ggna)
    first, other = means(g_gna[...].astype(F32), n_attn[...], gain_attn[...])
    back = sp_attn[:, 0:1] * (
        g_gna[:, cols(me)].astype(F32) * gain_attn[:, cols(me)]
        - first
        - n_attn[:, cols(me)] * other
    )
    o_bs[0] = (gs_ref[0].astype(F32) + back[0:length]).astype(BF)
    for k in range(2, bits):
        c_sm.wait_recv()
        sm_s[k] = sm_s[k - 1] + sm_r[k - 1]
        c_sm = send(sm_s.at[k], sm_r.at[k], partner[k], me)
        for p in (0, 1, 4, 3, 2, 5):
            zs[p] = merge(p, k, zs[p])
    c_sm.wait_recv()
    small = sm_s[bits - 1] + sm_r[bits - 1]
    o_ga[...] = small[:, 0:width]
    o_gm[...] = small[:, width : 2 * width]
    o_bias[...] = small[:, 2 * width :]
    for c in pending:
        c.wait_send()


def hand_out(*refs):
    count = (len(refs) - 2) // 3
    source, target, held = refs[:count], refs[count : 2 * count], refs[2 * count : 3 * count]
    first = [pltpu.make_async_copy(source[i], held[i], refs[-2].at[i]) for i in range(count)]
    second = [pltpu.make_async_copy(held[i], target[i], refs[-1].at[i]) for i in range(count)]
    for c in first:
        c.start()
    for c, e in zip(first, second):
        c.wait()
        e.start()
    for e in second:
        e.wait()


def on_device(
    out_first, out_second, grad_first, grad_second, gain_attn, gain_mlp,
    qkv_weight, proj_weight, inner_weight, inner_bias, outer_weight,
):
    images, length, width = out_first.shape
    parts = lax.axis_size("tensor")
    groups = lax.axis_size("dp")
    full = width * parts
    hid = inner_weight.shape[1]
    rows = (length + 15) // 16 * 16
    shard = full // groups
    bits = groups.bit_length() - 1
    sizes = (groups, length, width, full, hid, 256, rows)
    vm = pltpu.VMEM
    half = groups // 2
    scratch = [
        vm((3, full, width), BF), vm((full, width), BF), vm((full, hid), BF), vm((full, hid), BF),
    ]
    scratch += [vm((2, 2, rows, full), BF)] + [vm((rows, full), BF)] * 4
    scratch += [vm((rows, full), BF)] * 4
    scratch += [vm((rows, full), F32)] * 2 + [vm((rows, 128), F32)]
    scratch += [vm((rows, hid), F32), vm((rows, 3 * width), BF), vm((rows, width), BF)]
    scratch += [vm((2, half, 2, shard, rows), BF), vm((2, half, shard, rows), BF)]
    scratch += [vm((2, 2, half, shard, rows), BF), vm((half, 2, shard, rows), BF)]
    scratch += [vm((2, rows, hid), BF), vm((2, rows, hid), BF), vm((2, rows, width), BF), vm((3, 2, rows, width), BF)]
    scratch += [
        vm((4, 2, rows, width), BF), vm((4, 2, rows, width), BF), vm((4, 2, rows, width), F32),
        vm((4, rows, width), BF), vm((4, rows, width), BF),
    ]
    small = 2 * width + hid
    scratch += [vm((bits, 1, small), F32), vm((bits, 1, small), F32)]
    for n in (hid, hid, width, width, width, width):
        m = half
        bufs = []
        for k in range(m.bit_length() - 1):
            bufs += [vm((m // 2, 2, shard, n), F32), vm((m // 2, shard, n), BF), vm((m // 2, shard, n), BF)]
            m //= 2
        scratch.append(bufs)
    scratch += [pltpu.SemaphoreType.DMA((80,)), pltpu.SemaphoreType.DMA((80,)), pltpu.SemaphoreType.DMA((4,))]
    local = jax.ShapeDtypeStruct((images, length, width), BF)
    out_shape = [
        local, local, local, local,
        jax.ShapeDtypeStruct((3, shard, width), F32),
        jax.ShapeDtypeStruct((shard, width), F32),
        jax.ShapeDtypeStruct((shard, hid), F32),
        jax.ShapeDtypeStruct((1, width), F32),
        jax.ShapeDtypeStruct((1, width), F32),
        jax.ShapeDtypeStruct((1, hid), F32),
        jax.ShapeDtypeStruct((shard, hid), F32),
    ]
    v = pl.BlockSpec(memory_space=pltpu.VMEM)
    a = pl.BlockSpec(memory_space=pl.ANY)
    hbm = pl.BlockSpec(memory_space=pltpu.HBM)
    o = pl.pallas_call(
        functools.partial(kernel, sizes),
        out_shape=out_shape,
        in_specs=[v] * 7 + [hbm] * 4,
        out_specs=[v] * 11,
        scratch_shapes=scratch,
        compiler_params=pltpu.CompilerParams(
            collective_id=0, has_side_effects=True, vmem_limit_bytes=LIMIT
        ),
    )(
        out_first, out_second, grad_first, grad_second,
        gain_attn.reshape(1, full), gain_mlp.reshape(1, full), inner_bias.reshape(1, hid),
        jnp.transpose(qkv_weight, (1, 0, 2)), proj_weight, inner_weight, outer_weight,
    )
    o = pl.pallas_call(
        hand_out,
        out_shape=out_shape,
        in_specs=[a] * 11,
        out_specs=[a] * 11,
        scratch_shapes=[vm(x.shape, x.dtype) for x in out_shape]
        + [pltpu.SemaphoreType.DMA((11,)), pltpu.SemaphoreType.DMA((11,))],
        compiler_params=pltpu.CompilerParams(vmem_limit_bytes=LIMIT),
    )(*o)
    return (
        o[0], o[1], o[2], o[3], jnp.transpose(o[4], (1, 0, 2)), o[5], o[6],
        o[9].reshape(hid), o[10], o[7].reshape(width), o[8].reshape(width),
    )


def solution(mesh):
    act = P("dp", None, "tensor")
    in_specs = (
        act, act, act, act, P(), P(), P(None, None, "tensor"), P(None, "tensor"),
        P(None, "tensor"), P("tensor"), P(None, "tensor"),
    )
    out_specs = (
        act, act, act, act, P("dp", None, "tensor"), P("dp", "tensor"), P("dp", "tensor"),
        P("tensor"), P("dp", "tensor"), P("tensor"), P("tensor"),
    )
    return jax.shard_map(
        on_device, mesh=mesh, in_specs=in_specs, out_specs=out_specs, check_vma=False
    )
```
